32 devices in a mesh: blk: 8 (over z, y), col: 4 (over x, core).
Axes of the slice: x: 2, y: 2, z: 4, core: 2. Of those that a mesh axis runs over, the one named last changes fastest.
Arguments:
- spectra: bfloat16 [64, 128, 256], P(('blk', 'col')), may hold values from -5 to 5
- kernels: bfloat16 [60, 128, 256], replicated, may hold values from -5 to 5
- weights: float32 [60], replicated, may hold values from 0.3 to 1
- hotspot_flags: int32 [64], P(('blk', 'col')), may hold values from 0 to 1, as said below
- helper_map: int32 [64], P(('blk', 'col')), may hold values from 0 to 3, as said below
- kernel_counts: int32 [64], P(('blk', 'col')), may hold values from 6 to 12
Outputs:
- aerial_images: float32 [64, 256, 256], P(('blk', 'col'))
- pending: float32 [8, 4], P('blk', 'col')
The draws below stay inside these ranges and needn't reach their ends.
Inputs may be any that keep to these rules, and one draw needn't show every extreme that they name: `hotspot_flags`: some device has all its 2 tiles flagged in every draw. `helper_map`: among one device's flagged tiles at most 1 name the same value, and in every draw some device has exactly 1 flagged tiles naming one value.
All inputs are finite; a program needn't handle non-finite values.
Results may differ from the reference program's by a relative error of at most 0.0037.
Values may be sent and summed in bfloat16 or wider, within the bound.
No kernel may reach another device: no remote copies, remote signals or barrier semaphores. Data moves between devices by JAX's collectives and lax.ppermute only.
A program may use at most 64 MiB of HBM per device.

```python
import math
import jax
import jax.numpy as jnp
from jax import lax

P_SIZE = 128
Q = 256
KERN = 60
KBLOCK = 12
TILES_DEV = 2
CAP = 1
ROWS = 8
COLS = 4
TILES = 64


def joint_plan(key):
    folded = jax.random.fold_in(key, 31)
    subkeys = jax.random.split(folded, 7)
    device_total = ROWS * COLS
    device_ids = jnp.arange(device_total, dtype=jnp.int32)
    row_of = device_ids // COLS
    col_of = device_ids % COLS
    offsets = jax.random.randint(subkeys[0], (2,), 0, 4)
    candidate = (row_of % 4 == offsets[0]) & (col_of % 4 == offsets[1])
    coin = jax.random.randint(subkeys[1], (device_total,), 0, 2) == 0
    forced_pick = jax.random.randint(subkeys[2], (), 0, ROWS // 4 * (COLS // 4))
    forced_dev = (forced_pick // (COLS // 4) * 4 + offsets[0]) * COLS + forced_pick % (COLS // 4) * 4 + offsets[1]
    heavy_device = candidate & (coin | (device_ids == forced_dev))
    light = (jax.random.randint(subkeys[3], (device_total,), 0, 4) == 0).astype(jnp.int32)
    flag_count = jnp.where(heavy_device, TILES_DEV, jnp.minimum(light, TILES_DEV))
    scores = jax.random.randint(subkeys[4], (device_total, TILES_DEV), 0, 1 << 20) * TILES_DEV + jnp.arange(TILES_DEV)[None, :]
    tile_order = jnp.argsort(scores, axis=1)
    position = jnp.argsort(tile_order, axis=1)
    flagged = position < flag_count[:, None]
    dir_scores = jax.random.randint(subkeys[5], (device_total, 4), 0, 1 << 20) * 4 + jnp.arange(4)[None, :]
    dir_order = jnp.argsort(dir_scores, axis=1)
    slot_group = jnp.minimum(position // CAP, 3)
    chosen_dir = jnp.take_along_axis(dir_order, slot_group, axis=1)
    unused_route = jax.random.randint(subkeys[6], (device_total, TILES_DEV), 0, 4)
    route_values = jnp.where(flagged, chosen_dir, unused_route)
    return (flagged.astype(jnp.int32).reshape(-1), route_values.astype(jnp.int32).reshape(-1))


def draw_hotspot_flags(key, part):
    return joint_plan(key)[0]


def draw_helper_map(key, part):
    return joint_plan(key)[1]


def place_ends(array, key, least, high):
    longest = array.shape.index(max(array.shape))
    spots = []
    for shift in (0, 1):
        where = [jax.random.randint(jax.random.fold_in(key, axis), (), 0, length) for axis, length in enumerate(array.shape)]
        where[longest] = (where[longest] + shift) % array.shape[longest]
        spots.append(tuple(where))
    return array.at[spots[0]].set(least).at[spots[1]].set(high)


def level_of(stream_key, dims, pieces, smallest, top_value):
    loudness, own = 1.0, jax.random.fold_in(stream_key, 6)
    for axis_at, blocks in pieces:
        heights = jnp.exp(jax.random.uniform(jax.random.fold_in(own, axis_at), (blocks,), jnp.float32, smallest / len(pieces), top_value / len(pieces)))
        loudness = loudness * jnp.repeat(heights, dims[axis_at] // blocks).reshape([-1 if axis == axis_at else 1 for axis in range(len(dims))])
    return loudness


def centred(rng, shape, scale, bound, pieces=(), kind=jnp.bfloat16):
    entries = jax.random.normal(rng, shape, jnp.float32) * scale
    if len(pieces) > 0:
        entries = level_of(rng, shape, pieces, -0.22, 0.18) * entries
    return jnp.clip(entries, min=-bound, max=bound).astype(kind)


def setup_inputs(seed: int = 0) -> dict:
    seeds = jax.random.split(jax.random.key(seed), 7)
    spectra = centred(seeds[0], (TILES, P_SIZE, 2 * P_SIZE), 0.7, 5.0, ((0, 32),))
    kernels = centred(seeds[1], (KERN, P_SIZE, 2 * P_SIZE), 0.7, 5.0)
    weights = jnp.clip(jnp.exp(jax.random.uniform(seeds[2], (KERN,), jnp.float32, math.log(0.3), math.log(1.0))), 0.3, 1.0)
    hotspot_flags = draw_hotspot_flags(jax.random.fold_in(seeds[6], 71), 0)
    helper_map = draw_helper_map(jax.random.fold_in(seeds[6], 71), 0)
    kernel_counts = place_ends(jax.random.randint(seeds[5], (TILES,), KBLOCK // 2, KBLOCK + 1), jax.random.fold_in(seeds[5], 1), KBLOCK // 2, KBLOCK).astype(jnp.int32)
    return {"spectra": spectra, "kernels": kernels, "weights": weights, "hotspot_flags": hotspot_flags, "helper_map": helper_map, "kernel_counts": kernel_counts}


def make_tables(band_width, length):
    row_index = jnp.arange(length, dtype=jnp.int32)[:, None]
    col_index = jnp.arange(band_width, dtype=jnp.int32)[None, :] - band_width // 2
    phase_angle = jnp.mod(row_index * col_index, length).astype(jnp.float32) * (2.0 * math.pi / length)
    scale_factor = 1.0 / math.sqrt(band_width)
    real_part = (jnp.cos(phase_angle) * scale_factor).astype(jnp.bfloat16)
    imag_part = (jnp.sin(phase_angle) * scale_factor).astype(jnp.bfloat16)
    right_table = jnp.concatenate([jnp.concatenate([real_part.T, imag_part.T], 1), jnp.concatenate([-imag_part.T, real_part.T], 1)], 0)
    return (real_part, imag_part, right_table)

def tile_image(spectrum, kernels, weights, kernel_count, tables):
    real_part, imag_part, right_table = tables
    band_width = spectrum.shape[0]
    length = real_part.shape[0]
    spectrum_f = spectrum.astype(jnp.float32)
    spec_real = spectrum_f[:, :band_width]
    spec_imag = spectrum_f[:, band_width:]

    def add_block(block_index, accum):
        first_kernel = (block_index * KBLOCK).astype(jnp.int32)
        kernel_part = lax.dynamic_slice_in_dim(kernels, first_kernel, KBLOCK, 0).astype(jnp.float32)
        weight_part = lax.dynamic_slice_in_dim(weights, first_kernel, KBLOCK, 0)
        weight_part = jnp.where(first_kernel + jnp.arange(KBLOCK, dtype=jnp.int32) < kernel_count, weight_part, jnp.zeros_like(weight_part))
        kern_real = kernel_part[..., :band_width]
        kern_imag = kernel_part[..., band_width:]
        band = jnp.concatenate([kern_real * spec_real - kern_imag * spec_imag, kern_real * spec_imag + kern_imag * spec_real], -1).astype(jnp.bfloat16)
        half = jnp.dot(band.reshape(KBLOCK * band_width, 2 * band_width), right_table, preferred_element_type=jnp.float32)
        half = half.reshape(KBLOCK, band_width, 2 * length).astype(jnp.bfloat16)
        real_rows = jnp.einsum('qp,kpx->kqx', real_part.astype(jnp.float32), half.astype(jnp.float32))
        imag_rows = jnp.einsum('qp,kpx->kqx', imag_part.astype(jnp.float32), half.astype(jnp.float32))
        field_real = real_rows[..., :length] - imag_rows[..., length:]
        field_imag = real_rows[..., length:] + imag_rows[..., :length]
        intensity_part = field_real * field_real + field_imag * field_imag
        return accum + lax.optimization_barrier(jnp.sum(weight_part[:, None, None] * intensity_part, 0))
    blocks = ((kernel_count + KBLOCK - 1) // KBLOCK).astype(jnp.int32)
    accum = lax.fori_loop(jnp.int32(0), blocks, add_block, jnp.zeros((length, length), jnp.float32))
    weight_total = jnp.sum(jnp.where(jnp.arange(weights.shape[0], dtype=jnp.int32) < kernel_count, weights, jnp.zeros_like(weights)))
    return accum / weight_total

def reference(spectra, kernels, weights, hotspot_flags, helper_map, kernel_counts):
    tables = make_tables(P_SIZE, Q)
    flagged = hotspot_flags == 1
    numbers = jnp.where(flagged, KERN, kernel_counts).astype(jnp.int32)

    def one_tile(parcel):
        return tile_image(parcel[0], kernels, weights, parcel[1], tables)
    aerial_images = lax.map(one_tile, (spectra, numbers))
    device = (jnp.arange(TILES, dtype=jnp.int32) // TILES_DEV).astype(jnp.int32)
    device_row = device // COLS
    device_col = device % COLS
    row_shift = jnp.where(helper_map == 0, 1, jnp.where(helper_map == 1, -1, 0)).astype(jnp.int32)
    col_shift = jnp.where(helper_map == 2, 1, jnp.where(helper_map == 3, -1, 0)).astype(jnp.int32)
    helper = (jnp.mod(device_row + row_shift, ROWS) * COLS + jnp.mod(device_col + col_shift, COLS)).astype(jnp.int32)
    target = jnp.where(flagged, helper, device).astype(jnp.int32)
    amount = numbers.astype(jnp.float32)
    pending = jax.ops.segment_sum(amount, target, num_segments=ROWS * COLS).reshape(ROWS, COLS) / KERN
    return (aerial_images, pending)
```

```python
import math

import jax
import jax.numpy as jnp
import numpy as np
from jax import lax
from jax.experimental import pallas as pl
from jax.experimental.pallas import tpu as pltpu
from jax.sharding import PartitionSpec as P

Q = 256
KB = 6


def make_table(band_width, length):
    row_index = np.arange(length, dtype=np.int32)[:, None]
    col_index = np.arange(band_width, dtype=np.int32)[None, :] - band_width // 2
    angle = np.mod(row_index * col_index, length).astype(np.float64) * (2.0 * math.pi / length)
    scale = 1.0 / math.sqrt(band_width)
    real = (np.cos(angle) * scale).astype(np.float32).T
    imag = (np.sin(angle) * scale).astype(np.float32).T
    table = np.block([[real, imag], [-imag, real]])
    return jnp.asarray(table).astype(jnp.bfloat16)


def tile_kernel(counts, w_smem, w_vec, spectra, kernels, table, out, kbuf, sbuf, sf, tbuf, img, ksem, ssem, tsem, osem):
    tiles, width, _ = spectra.shape
    length = out.shape[1]
    kern_total = kernels.shape[0]
    blocks_max = kern_total // KB
    table_copy = pltpu.make_async_copy(table, tbuf, tsem)
    table_copy.start()
    spectra_copy = pltpu.make_async_copy(spectra, sbuf, ssem)
    spectra_copy.start()
    n0 = counts[0]
    n1 = counts[1]
    nb0 = (n0 + KB - 1) // KB
    nb1 = (n1 + KB - 1) // KB
    total = nb0 + nb1
    needed = jnp.maximum(nb0, nb1)

    def chunk(b):
        part = pl.ds(b * KB, KB)
        return pltpu.make_async_copy(kernels.at[part], kbuf.at[part], ksem.at[b])

    def start_chunk(b, _):
        chunk(b).start()
        return _

    lax.fori_loop(0, needed, start_chunk, 0)
    img[...] = jnp.zeros_like(img)
    spectra_copy.wait()
    sf[...] = sbuf[...].astype(jnp.float32)
    table_copy.wait()

    def place(i):
        second = i >= nb0
        t = jnp.where(second, 1, 0).astype(jnp.int32)
        b = jnp.where(second, i - nb0, i)
        n = jnp.where(second, n1, n0)
        return t, b, n

    def body(*accs):
        a0, a1, b0, b1 = accs[0:3], accs[3:6], accs[6:8], accs[8:10]
        pltpu.matmul_push_rhs(tbuf[:, :length], staging_register=0, mxu_index=0)
        pltpu.matmul_push_rhs(tbuf[:, length:], staging_register=0, mxu_index=1)
        zero = jnp.zeros((16, 2 * width), jnp.bfloat16)
        for acc in accs:
            pltpu.matmul_pop(acc)

        def stage_one(t, k, j, first=False):
            kb = kbuf[k].astype(jnp.float32)
            kr, ki = kb[:, :width], kb[:, width:]
            sr, si = sf[t, :, :width], sf[t, :, width:]
            band = jnp.concatenate([kr * sr - ki * si, kr * si + ki * sr], 1).astype(jnp.bfloat16)
            load = 0 if first else None
            pltpu.matmul_acc_lhs(a0[j], band, load_staged_rhs=load)
            pltpu.matmul_acc_lhs(a1[j], band, load_staged_rhs=load)

        def middle(j):
            hr = pltpu.matmul_pop(a0[j]).astype(jnp.bfloat16)
            hi = pltpu.matmul_pop(a1[j]).astype(jnp.bfloat16)
            return jnp.concatenate([hr.T, hi.T], 1)

        def stage_two(half, j):
            pltpu.matmul_acc_lhs(b0[j], half)
            pltpu.matmul_acc_lhs(b1[j], half)

        def finish(t, w, j):
            fr = pltpu.matmul_pop(b0[j])
            fi = pltpu.matmul_pop(b1[j])
            img[t] = img[t] + w * (fr * fr + fi * fi)

        t, b, n = place(0)
        chunk(0).wait()
        stage_one(t, b * KB, 0, first=True)
        stage_one(t, b * KB + 1, 1)

        def block(i, carry):
            t, b, n = place(i)
            tn, bn, _ = place(jnp.minimum(i + 1, total - 1))
            kn = bn * KB
            fresh = (bn > waited_of(carry))

            @pl.when(fresh)
            def _():
                chunk(bn).wait()

            for u in range(KB):
                half = middle(u % 3)
                if u + 2 < KB:
                    stage_one(t, b * KB + u + 2, (u + 2) % 3)
                else:
                    stage_one(tn, kn + (u + 2 - KB), (u + 2) % 3)
                stage_two(half, u % 2)
                if u > 0:
                    k = b * KB + u - 1
                    finish(t, jnp.where(k < n, w_smem[k], 0.0), (u - 1) % 2)
            k = b * KB + KB - 1
            finish(t, jnp.where(k < n, w_smem[k], 0.0), (KB - 1) % 2)
            return jnp.maximum(carry, bn)

        def waited_of(carry):
            return carry

        lax.fori_loop(0, total, block, jnp.int32(0))
        for j in range(3):
            pltpu.matmul_pop(a0[j])
            pltpu.matmul_pop(a1[j])

    pl.run_scoped(
        body,
        *[pltpu.ACC(0)((width, length), jnp.float32)] * 3,
        *[pltpu.ACC(1)((width, length), jnp.float32)] * 3,
        *[pltpu.ACC(0)((length, length), jnp.float32)] * 2,
        *[pltpu.ACC(1)((length, length), jnp.float32)] * 2,
    )
    lane = lax.broadcasted_iota(jnp.int32, w_vec.shape, 1)
    for t in range(tiles):
        weight = jnp.sum(jnp.where(lane < counts[t], w_vec[...], 0.0), axis=1, keepdims=True)
        out[t] = img[t].T * (1.0 / weight)


def images_of(counts, weights, spectra, kernels, table):
    tiles, width, _ = spectra.shape
    kern_total = kernels.shape[0]
    smem = pl.BlockSpec(memory_space=pltpu.SMEM)
    vmem = pl.BlockSpec(memory_space=pltpu.VMEM)
    hbm = pl.BlockSpec(memory_space=pltpu.HBM)
    return pl.pallas_call(
        tile_kernel,
        out_shape=jax.ShapeDtypeStruct((tiles, Q, Q), jnp.float32),
        in_specs=[smem, smem, vmem, hbm, hbm, hbm],
        out_specs=vmem,
        scratch_shapes=[
            pltpu.VMEM(kernels.shape, jnp.bfloat16),
            pltpu.VMEM(spectra.shape, jnp.bfloat16),
            pltpu.VMEM(spectra.shape, jnp.float32),
            pltpu.VMEM(table.shape, jnp.bfloat16),
            pltpu.VMEM((tiles, Q, Q), jnp.float32),
            pltpu.SemaphoreType.DMA((kern_total // KB,)),
            pltpu.SemaphoreType.DMA,
            pltpu.SemaphoreType.DMA,
            pltpu.SemaphoreType.DMA,
        ],
        name="tiles",
    )(counts, weights, weights.reshape(1, -1), spectra, kernels, table)


def on_device(spectra, kernels, weights, hotspot_flags, helper_map, kernel_counts):
    kernel_total = kernels.shape[0]
    flagged = hotspot_flags == 1
    numbers = jnp.where(flagged, kernel_total, kernel_counts)
    table = make_table(spectra.shape[1], Q)
    aerial = images_of(numbers, weights, spectra, kernels, table)

    amounts = numbers.astype(jnp.float32)

    def handed(direction):
        return jnp.sum(jnp.where(flagged & (helper_map == direction), amounts, 0.0)).reshape(1, 1)

    rows, cols = lax.axis_size("blk"), lax.axis_size("col")
    up = [(i, (i + 1) % rows) for i in range(rows)]
    down = [(j, i) for i, j in up]
    right = [(i, (i + 1) % cols) for i in range(cols)]
    left = [(j, i) for i, j in right]
    got = [
        lax.ppermute(handed(0), "blk", up),
        lax.ppermute(handed(1), "blk", down),
        lax.ppermute(handed(2), "col", right),
        lax.ppermute(handed(3), "col", left),
    ]
    kept = jnp.sum(jnp.where(flagged, 0.0, amounts)).reshape(1, 1)
    pending = (kept + got[0] + got[1] + got[2] + got[3]) / kernel_total
    return aerial, pending


def solution(mesh):
    in_specs = (
        P(("blk", "col"), None, None),
        P(),
        P(),
        P(("blk", "col")),
        P(("blk", "col")),
        P(("blk", "col")),
    )
    out_specs = (P(("blk", "col"), None, None), P("blk", "col"))
    return jax.shard_map(on_device, mesh=mesh, in_specs=in_specs, out_specs=out_specs, check_vma=False)
```

```python
import math

import jax
import jax.numpy as jnp
import numpy as np
from jax import lax
from jax.experimental import pallas as pl
from jax.experimental.pallas import tpu as pltpu
from jax.sharding import PartitionSpec as P

Q = 256
KB = 6


def make_table(band_width, length):
    row_index = np.arange(length, dtype=np.int32)[:, None]
    col_index = np.arange(band_width, dtype=np.int32)[None, :] - band_width // 2
    angle = np.mod(row_index * col_index, length).astype(np.float64) * (2.0 * math.pi / length)
    scale = 1.0 / math.sqrt(band_width)
    real = (np.cos(angle) * scale).astype(np.float32).T
    imag = (np.sin(angle) * scale).astype(np.float32).T
    table = np.block([[real, imag], [-imag, real]])
    return jnp.asarray(table).astype(jnp.bfloat16)


def tile_kernel(flags, counts, weights, spectra, kernels, table, out, fl, cn, wv, ws, kbuf, sbuf, sf, tbuf, img, half, ksem, ssem, tsem, fsem, csem, wsem, vsem, osem):
    tiles, width, _ = spectra.shape
    length = out.shape[1]
    kern_total = kernels.shape[0]
    flag_copy = pltpu.make_async_copy(flags, fl, fsem)
    count_copy = pltpu.make_async_copy(counts, cn, csem)
    table_copy = pltpu.make_async_copy(table, tbuf, tsem)
    spectra_copy = pltpu.make_async_copy(spectra, sbuf, ssem)
    scalar_copy = pltpu.make_async_copy(weights, ws, wsem)
    vector_copy = pltpu.make_async_copy(weights, wv, vsem)

    def chunk(b):
        part = pl.ds(b * KB, KB)
        return pltpu.make_async_copy(kernels.at[part], kbuf.at[part], ksem.at[b])

    flag_copy.start()
    count_copy.start()
    spectra_copy.start()
    chunk(0).start()
    table_copy.start()
    scalar_copy.start()
    vector_copy.start()
    img[...] = jnp.zeros_like(img)

    def body(*accs):
        a0, a1, b0, b1 = accs[0:2], accs[2:4], accs[4:7], accs[7:10]
        for acc in accs:
            pltpu.matmul_pop(acc)
        flag_copy.wait()
        count_copy.wait()
        n0 = jnp.where(fl[0] == 1, kern_total, cn[0])
        n1 = jnp.where(fl[1] == 1, kern_total, cn[1])
        nb0 = (n0 + KB - 1) // KB
        nb1 = (n1 + KB - 1) // KB
        total = nb0 + nb1

        def start_chunk(b, c):
            chunk(b).start()
            return c

        lax.fori_loop(1, jnp.maximum(nb0, nb1), start_chunk, 0)

        def place(i):
            second = i >= nb0
            t = jnp.where(second, 1, 0).astype(jnp.int32)
            b = jnp.where(second, i - nb0, i)
            n = jnp.where(second, n1, n0)
            return t, b, n

        spectra_copy.wait()
        sf[...] = sbuf[...].astype(jnp.float32)
        chunk(0).wait()
        table_copy.wait()
        pltpu.matmul_push_rhs(tbuf[:, :length], staging_register=0, mxu_index=0)
        pltpu.matmul_push_rhs(tbuf[:, length:], staging_register=0, mxu_index=1)

        def stage_one(t, k, j, first=False):
            kb = kbuf[k].astype(jnp.float32)
            kr, ki = kb[:, :width], kb[:, width:]
            sr, si = sf[t, :, :width], sf[t, :, width:]
            band = jnp.concatenate([kr * sr - ki * si, kr * si + ki * sr], 1).astype(jnp.bfloat16)
            load = 0 if first else None
            pltpu.matmul_acc_lhs(a0[j], band, load_staged_rhs=load)
            pltpu.matmul_acc_lhs(a1[j], band, load_staged_rhs=load)

        def middle(j):
            hr = pltpu.matmul_pop(a0[j]).astype(jnp.bfloat16)
            hi = pltpu.matmul_pop(a1[j]).astype(jnp.bfloat16)
            return jnp.concatenate([hr.T, hi.T], 1)

        def stage_two(data, j):
            pltpu.matmul_acc_lhs(b0[j], data)
            pltpu.matmul_acc_lhs(b1[j], data)

        def finish(t, k, n, j):
            w = jnp.where(k < n, ws[0, k], 0.0)
            fr = pltpu.matmul_pop(b0[j])
            fi = pltpu.matmul_pop(b1[j])
            img[t] = img[t] + w * (fr * fr + fi * fi)

        scalar_copy.wait()
        vector_copy.wait()
        t, b, n = place(0)
        stage_one(t, 0, 0, first=True)
        stage_one(t, 1, 1)
        half[...] = middle(0)

        def block(i, waited):
            t, b, n = place(i)
            tn, bn, _ = place(jnp.minimum(i + 1, total - 1))
            tp, bp, np_ = place(jnp.maximum(i - 1, 0))

            @pl.when(bn > waited)
            def _():
                chunk(bn).wait()

            data = half[...]
            for u in range(KB):
                if u + 2 < KB:
                    stage_one(t, b * KB + u + 2, u % 2)
                else:
                    stage_one(tn, bn * KB + (u + 2 - KB), u % 2)
                stage_two(data, u % 3)
                data = middle((u + 1) % 2)
                if u < 2:
                    finish(tp, bp * KB + KB - 2 + u, np_, (u + 1) % 3)
                else:
                    finish(t, b * KB + u - 2, n, (u + 1) % 3)
            half[...] = data
            return jnp.maximum(waited, bn)

        lax.fori_loop(0, total, block, jnp.int32(0))
        t, b, n = place(total - 1)
        finish(t, b * KB + KB - 2, n, 1)
        finish(t, b * KB + KB - 1, n, 2)
        pltpu.matmul_pop(a0[1])
        pltpu.matmul_pop(a1[1])
        lane = lax.broadcasted_iota(jnp.int32, (1, kern_total), 1)
        numbers = (n0, n1)
        for t in range(tiles):
            weight = jnp.sum(jnp.where(lane < numbers[t], wv[...], 0.0), axis=1, keepdims=True)
            out[t] = img[t].T * (1.0 / weight)

    pl.run_scoped(
        body,
        *[pltpu.ACC(0)((width, length), jnp.float32)] * 2,
        *[pltpu.ACC(1)((width, length), jnp.float32)] * 2,
        *[pltpu.ACC(0)((length, length), jnp.float32)] * 3,
        *[pltpu.ACC(1)((length, length), jnp.float32)] * 3,
    )


def images_of(flags, counts, weights, spectra, kernels, table):
    tiles, width, _ = spectra.shape
    kern_total = kernels.shape[0]
    vmem = pl.BlockSpec(memory_space=pltpu.VMEM)
    hbm = pl.BlockSpec(memory_space=pltpu.HBM)
    return pl.pallas_call(
        tile_kernel,
        out_shape=jax.ShapeDtypeStruct((tiles, Q, Q), jnp.float32),
        in_specs=[hbm] * 6,
        out_specs=vmem,
        scratch_shapes=[
            pltpu.SMEM((tiles,), jnp.int32),
            pltpu.SMEM((tiles,), jnp.int32),
            pltpu.VMEM((1, kern_total), jnp.float32),
            pltpu.SMEM((1, kern_total), jnp.float32),
            pltpu.VMEM(kernels.shape, jnp.bfloat16),
            pltpu.VMEM(spectra.shape, jnp.bfloat16),
            pltpu.VMEM(spectra.shape, jnp.float32),
            pltpu.VMEM(table.shape, jnp.bfloat16),
            pltpu.VMEM((tiles, Q, Q), jnp.float32),
            pltpu.VMEM((Q, 2 * width), jnp.bfloat16),
            pltpu.SemaphoreType.DMA((kern_total // KB,)),
            *[pltpu.SemaphoreType.DMA] * 7,
        ],
        name="tiles",
    )(flags, counts, weights.reshape(1, -1), spectra, kernels, table)


def on_device(spectra, kernels, weights, hotspot_flags, helper_map, kernel_counts):
    kernel_total = kernels.shape[0]
    flagged = hotspot_flags == 1
    numbers = jnp.where(flagged, kernel_total, kernel_counts)
    table = make_table(spectra.shape[1], Q)
    aerial = images_of(hotspot_flags, kernel_counts, weights, spectra, kernels, table)

    amounts = numbers.astype(jnp.float32)

    def handed(direction):
        return jnp.sum(jnp.where(flagged & (helper_map == direction), amounts, 0.0)).reshape(1, 1)

    rows, cols = lax.axis_size("blk"), lax.axis_size("col")
    up = [(i, (i + 1) % rows) for i in range(rows)]
    down = [(j, i) for i, j in up]
    right = [(i, (i + 1) % cols) for i in range(cols)]
    left = [(j, i) for i, j in right]
    got = [
        lax.ppermute(handed(0), "blk", up),
        lax.ppermute(handed(1), "blk", down),
        lax.ppermute(handed(2), "col", right),
        lax.ppermute(handed(3), "col", left),
    ]
    kept = jnp.sum(jnp.where(flagged, 0.0, amounts)).reshape(1, 1)
    pending = (kept + got[0] + got[1] + got[2] + got[3]) / kernel_total
    return aerial, pending


def solution(mesh):
    in_specs = (
        P(("blk", "col"), None, None),
        P(),
        P(),
        P(("blk", "col")),
        P(("blk", "col")),
        P(("blk", "col")),
    )
    out_specs = (P(("blk", "col"), None, None), P("blk", "col"))
    return jax.shard_map(on_device, mesh=mesh, in_specs=in_specs, out_specs=out_specs, check_vma=False)
```

```python
import math

import jax
import jax.numpy as jnp
import numpy as np
from jax import lax
from jax.experimental import pallas as pl
from jax.experimental.pallas import tpu as pltpu
from jax.sharding import PartitionSpec as P

Q = 256
KB = 6


def make_table(band_width, length):
    row_index = np.arange(length, dtype=np.int32)[:, None]
    col_index = np.arange(band_width, dtype=np.int32)[None, :] - band_width // 2
    angle = np.mod(row_index * col_index, length).astype(np.float64) * (2.0 * math.pi / length)
    scale = 1.0 / math.sqrt(band_width)
    real = (np.cos(angle) * scale).astype(np.float32).T
    imag = (np.sin(angle) * scale).astype(np.float32).T
    table = np.block([[real, imag], [-imag, real]])
    return jnp.asarray(table).astype(jnp.bfloat16)


def plan(core, flags, counts, kern_total):
    numbers, firsts, starts = [], [], [jnp.int32(0)]
    most = jnp.int32(0)
    for f, c in zip(flags, counts):
        for t in range(f.shape[0]):
            n = jnp.where(f[t] == 1, kern_total, c[t])
            first = lax.rem(core + t, 2)
            blocks = (n + KB - 1) // KB
            most = jnp.maximum(most, blocks)
            numbers.append(n)
            firsts.append(first)
            starts.append(starts[-1] + (blocks - first + 1) // 2)
    return numbers, firsts, starts, most


def run_blocks(low, high, lists, kbuf, tbuf, both, ws, img, half, accs, prepare, ready, ahead):
    numbers, firsts, starts, _ = lists
    width, length = kbuf.shape[1], img.shape[1]
    a0, a1, b0, b1 = accs[0:2], accs[2:4], accs[4:7], accs[7:10]

    def place(i):
        j, start, first, n = jnp.int32(0), starts[0], firsts[0], numbers[0]
        for q in range(1, len(numbers)):
            take = i >= starts[q]
            j = jnp.where(take, q, j)
            start = jnp.where(take, starts[q], start)
            first = jnp.where(take, firsts[q], first)
            n = jnp.where(take, numbers[q], n)
        return j, first + 2 * (i - start), n

    def stage_one(j, k, slot, first=False):
        kb = kbuf[k].astype(jnp.float32)
        kr, ki = kb[:, :width], kb[:, width:]
        sp = both[j].astype(jnp.float32)
        sr, si = sp[:, :width], sp[:, width:]
        band = jnp.concatenate([kr * sr - ki * si, kr * si + ki * sr], 1).astype(jnp.bfloat16)
        load = 0 if first else None
        pltpu.matmul_acc_lhs(a0[slot], band, load_staged_rhs=load)
        pltpu.matmul_acc_lhs(a1[slot], band, load_staged_rhs=load)

    def middle(slot):
        hr = pltpu.matmul_pop(a0[slot]).astype(jnp.bfloat16)
        hi = pltpu.matmul_pop(a1[slot]).astype(jnp.bfloat16)
        return jnp.concatenate([hr.T, hi.T], 1)

    def stage_two(data, slot):
        pltpu.matmul_acc_lhs(b0[slot], data)
        pltpu.matmul_acc_lhs(b1[slot], data)

    def finish(j, k, n, slot):
        w = jnp.where(k < n, ws[0, k], 0.0)
        fr = pltpu.matmul_pop(b0[slot])
        fi = pltpu.matmul_pop(b1[slot])
        img[j] = img[j] + w * (fr * fr + fi * fi)

    prepare()
    pltpu.matmul_push_rhs(tbuf[:, :length], staging_register=0, mxu_index=0)
    pltpu.matmul_push_rhs(tbuf[:, length:], staging_register=0, mxu_index=1)
    j, b, _ = place(low)
    stage_one(j, b * KB, 0, first=True)
    stage_one(j, b * KB + 1, 1)
    half[...] = middle(0)

    def block(i, here):
        j, b, n = place(i)
        jn, bn, _ = place(jnp.minimum(i + 1, high - 1))
        jp, bp, np_ = place(jnp.maximum(i - 1, low))
        if ready is not None:

            @pl.when(bn >= here)
            def _():
                lax.fori_loop(here, bn + 1, ready, 0)

        data = half[...]
        for u in range(KB):
            if u + 2 < KB:
                stage_one(j, b * KB + u + 2, u % 2)
            else:
                stage_one(jn, bn * KB + (u + 2 - KB), u % 2)
            stage_two(data, u % 3)
            data = middle((u + 1) % 2)
            if u < 2:
                finish(jp, bp * KB + KB - 2 + u, np_, (u + 1) % 3)
            else:
                finish(j, b * KB + u - 2, n, (u + 1) % 3)
        half[...] = data
        return jnp.maximum(here, bn + 1)

    here = lax.fori_loop(low, high, block, jnp.int32(ahead))
    j, b, n = place(jnp.maximum(high - 1, low))
    finish(j, b * KB + KB - 2, n, 1)
    finish(j, b * KB + KB - 1, n, 2)
    pltpu.matmul_pop(a0[1])
    pltpu.matmul_pop(a1[1])
    return here


def with_accs(body, width, length):
    pl.run_scoped(
        body,
        *[pltpu.ACC(0)((width, length), jnp.float32)] * 2,
        *[pltpu.ACC(1)((width, length), jnp.float32)] * 2,
        *[pltpu.ACC(0)((length, length), jnp.float32)] * 3,
        *[pltpu.ACC(1)((length, length), jnp.float32)] * 3,
    )


def first_kernel(pflags, pcounts, phelper, pspectra, flags, counts, helper, weights, spectra, kernels, table,
                 img, kbuf, tbuf, both, across, above, below, base, fl, cn, hm, ws, half, ksem, sems):
    tiles, width, _ = spectra.shape
    length = img.shape[1]
    kern_total = kernels.shape[0]
    core = lax.rem(lax.axis_index("col"), 2)
    pairs = [(flags, fl), (counts, cn), (helper, hm), (weights, ws), (table, tbuf), (spectra, both.at[pl.ds(0, tiles)])]
    copies = [pltpu.make_async_copy(src, dst, sems.at[i]) for i, (src, dst) in enumerate(pairs)]

    def chunk(b):
        part = pl.ds(b * KB, KB)
        return pltpu.make_async_copy(kernels.at[part], kbuf.at[part], ksem.at[b])

    def start_chunk(b, c):
        chunk(b).start()
        return c

    def wait_chunk(b, c):
        chunk(b).wait()
        return c

    for copy in copies:
        copy.start()
    for b in range(2):
        chunk(b).start()
    img[...] = jnp.zeros_like(img)
    both[tiles:] = pspectra[...]

    def body(*accs):
        for acc in accs:
            pltpu.matmul_pop(acc)
        for copy in copies[:3]:
            copy.wait()
        lists = plan(core, (fl, pflags), (cn, pcounts), kern_total)
        _, _, starts, most = lists
        lax.fori_loop(2, most, start_chunk, 0)
        odd_row = lax.rem(lax.axis_index("blk"), 2)

        def handed(f, h, direction):
            value = jnp.float32(0)
            for t in range(tiles):
                value = value + jnp.where((f[t] == 1) & (h[t] == direction), jnp.float32(kern_total), 0.0)
            return value

        across[...] = jnp.full(across.shape, handed(fl, hm, 3 - core))
        above[...] = jnp.full(above.shape, handed(fl, hm, odd_row))
        below[...] = jnp.full(below.shape, handed(fl, hm, 1 - odd_row))
        kept = handed(pflags, phelper, 3 - core)
        for t in range(tiles):
            kept = kept + jnp.where(fl[t] == 1, 0, cn[t]).astype(jnp.float32)
        base[...] = jnp.full(base.shape, kept)

        def prepare():
            for copy in copies[3:]:
                copy.wait()
            for b in range(2):
                chunk(b).wait()

        split = (2 * starts[-1] + 2) // 3
        here = run_blocks(jnp.int32(0), split, lists, kbuf, tbuf, both, ws, img, half, accs, prepare, wait_chunk, 2)
        lax.fori_loop(here, most, wait_chunk, 0)

    with_accs(body, width, length)


def second_kernel(pflags, pcounts, flags, counts, weights, kbuf, tbuf, both, img_in, own_out, peer_out,
                  fl, cn, ws, wv, half, img, sems):
    tiles = own_out.shape[0]
    kern_total, width, _ = kbuf.shape
    length = img.shape[1]
    core = lax.rem(lax.axis_index("col"), 2)
    pairs = [(flags, fl), (counts, cn), (weights, ws), (weights, wv)]
    copies = [pltpu.make_async_copy(src, dst, sems.at[i]) for i, (src, dst) in enumerate(pairs)]
    for copy in copies:
        copy.start()
    img[...] = img_in[...]

    def body(*accs):
        for acc in accs:
            pltpu.matmul_pop(acc)
        for copy in copies:
            copy.wait()
        lists = plan(core, (fl, pflags), (cn, pcounts), kern_total)
        numbers, _, starts, _ = lists
        split = (2 * starts[-1] + 2) // 3
        run_blocks(split, starts[-1], lists, kbuf, tbuf, both, ws, img, half, accs, lambda: None, None, 0)
        lane = lax.broadcasted_iota(jnp.int32, (1, kern_total), 1)
        for j in range(2 * tiles):
            weight = jnp.sum(jnp.where(lane < numbers[j], wv[...], 0.0), axis=1, keepdims=True)
            dest = own_out if j < tiles else peer_out
            dest[j % tiles] = img[j].T * (1.0 / weight)

    with_accs(body, width, length)


def on_device(spectra, kernels, weights, hotspot_flags, helper_map, kernel_counts):
    tiles, width, _ = spectra.shape
    kern_total = kernels.shape[0]
    rows, cols = lax.axis_size("blk"), lax.axis_size("col")
    table = make_table(width, Q)

    def pairs(size, first):
        return [p for i in range(first, size, 2) for p in ((i, (i + 1) % size), ((i + 1) % size, i))]

    twin = pairs(cols, 0)
    pspectra = lax.ppermute(spectra, "col", twin)
    pflags = lax.ppermute(hotspot_flags, "col", twin)
    pcounts = lax.ppermute(kernel_counts, "col", twin)
    phelper = lax.ppermute(helper_map, "col", twin)

    smem = pl.BlockSpec(memory_space=pltpu.SMEM)
    vmem = pl.BlockSpec(memory_space=pltpu.VMEM)
    hbm = pl.BlockSpec(memory_space=pltpu.HBM)

    def far(*arrays):
        return [pltpu.with_memory_space_constraint(x, pltpu.HBM) for x in arrays]

    f32, bf16 = jnp.float32, jnp.bfloat16
    image = jax.ShapeDtypeStruct((tiles, Q, Q), f32)
    images = jax.ShapeDtypeStruct((2 * tiles, Q, Q), f32)
    wide = jax.ShapeDtypeStruct((8, 128), f32)
    wrow = weights.reshape(1, -1)
    ints = pltpu.SMEM((tiles,), jnp.int32)
    row_smem = pltpu.SMEM((1, kern_total), f32)
    params = pltpu.CompilerParams(vmem_limit_bytes=16 * 2**20)
    half = pltpu.VMEM((Q, 2 * width), bf16)
    cost = pl.CostEstimate(flops=10**10, transcendentals=0, bytes_accessed=10**6)
    img, kbuf, tbuf, both, across, above, below, base = pl.pallas_call(
        first_kernel,
        out_shape=[
            images,
            jax.ShapeDtypeStruct(kernels.shape, bf16),
            jax.ShapeDtypeStruct(table.shape, bf16),
            jax.ShapeDtypeStruct((2 * tiles, width, 2 * width), bf16),
        ]
        + [wide] * 4,
        in_specs=[smem] * 3 + [vmem] + [hbm] * 7,
        out_specs=[vmem] * 8,
        scratch_shapes=[
            ints,
            ints,
            ints,
            row_smem,
            half,
            pltpu.SemaphoreType.DMA((kern_total // KB,)),
            pltpu.SemaphoreType.DMA((6,)),
        ],
        compiler_params=params,
        cost_estimate=cost,
        name="first",
    )(pflags, pcounts, phelper, pspectra, *far(hotspot_flags, kernel_counts, helper_map, wrow, spectra, kernels, table))
    got = [lax.ppermute(below, "blk", pairs(rows, 1))]
    got.append(lax.ppermute(above, "blk", pairs(rows, 0)))
    got.append(lax.ppermute(across, "col", pairs(cols, 1)))
    rest = pl.pallas_call(
        second_kernel,
        out_shape=[image, image],
        in_specs=[smem] * 2 + [hbm] * 3 + [vmem] * 4,
        out_specs=[vmem] * 2,
        scratch_shapes=[
            ints,
            ints,
            row_smem,
            pltpu.VMEM((1, kern_total), f32),
            half,
            pltpu.VMEM((2 * tiles, Q, Q), f32),
            pltpu.SemaphoreType.DMA((4,)),
        ],
        compiler_params=params,
        cost_estimate=cost,
        name="second",
    )
    own, peer = rest(pflags, pcounts, *far(hotspot_flags, kernel_counts, wrow), kbuf, tbuf, both, img)
    other = lax.ppermute(peer, "col", twin)
    pending = jnp.max((base + got[0] + got[1] + got[2]) / kern_total, keepdims=True)
    return own + other, pending


def solution(mesh):
    in_specs = (
        P(("blk", "col"), None, None),
        P(),
        P(),
        P(("blk", "col")),
        P(("blk", "col")),
        P(("blk", "col")),
    )
    out_specs = (P(("blk", "col"), None, None), P("blk", "col"))
    return jax.shard_map(on_device, mesh=mesh, in_specs=in_specs, out_specs=out_specs, check_vma=False)
```

```python
import functools
import math

import jax
import jax.numpy as jnp
import numpy as np
from jax import lax
from jax.experimental import pallas as pl
from jax.experimental.pallas import tpu as pltpu
from jax.sharding import PartitionSpec as P

Q = 256
KB = 6


def make_table(band_width, length):
    row_index = np.arange(length, dtype=np.int32)[:, None]
    col_index = np.arange(band_width, dtype=np.int32)[None, :] - band_width // 2
    angle = np.mod(row_index * col_index, length).astype(np.float64) * (2.0 * math.pi / length)
    scale = 1.0 / math.sqrt(band_width)
    real = (np.cos(angle) * scale).astype(np.float32).T
    imag = (np.sin(angle) * scale).astype(np.float32).T
    table = np.block([[real, imag], [-imag, real]])
    return jnp.asarray(table).astype(jnp.bfloat16)


def plan(core, flags, counts, kern_total):
    tiles, numbers, firsts, starts = [], [], [], [jnp.int32(0)]
    most = jnp.int32(0)
    for group, (f, c) in enumerate(zip(flags, counts)):
        per = f.shape[0]
        for q in range(per):
            t = lax.rem(core + q, per)
            n = jnp.where(f[t] == 1, kern_total, c[t])
            first = q % 2
            blocks = (n + KB - 1) // KB
            most = jnp.maximum(most, blocks)
            tiles.append(group * per + t)
            numbers.append(n)
            firsts.append(first)
            starts.append(starts[-1] + (blocks - first + 1) // 2)
    return tiles, numbers, firsts, starts, most


def fetch_kernel(flags, counts, helper, weights, spectra, kernels, table, fv, cv, hv, wv, kpart, tbuf, sbuf, sems):
    pairs = [(flags, fv), (counts, cv), (helper, hv), (weights, wv)]
    pairs += [(spectra, sbuf), (kernels.at[pl.ds(0, kpart.shape[0])], kpart), (table, tbuf)]
    copies = [pltpu.make_async_copy(src, dst, sems.at[i]) for i, (src, dst) in enumerate(pairs)]
    for copy in copies:
        copy.start()
    for copy in copies:
        copy.wait()


def split_of(total):
    return total - jnp.maximum((total - 2) // 2, 1)


def run_part(low, high, lists, kbuf, both, ws, img, half, accs, wait):
    a0, a1, b0, b1 = accs[0:2], accs[2:4], accs[4:7], accs[7:10]
    places, numbers, firsts, starts, _ = lists

    def place(i):
        j, start, first, n = places[0], starts[0], firsts[0], numbers[0]
        for q in range(1, len(numbers)):
            take = i >= starts[q]
            j = jnp.where(take, places[q], j)
            start = jnp.where(take, starts[q], start)
            first = jnp.where(take, firsts[q], first)
            n = jnp.where(take, numbers[q], n)
        return j, first + 2 * (i - start), n

    def finish(j, k, n, slot):
        w = jnp.where(k < n, ws[0, k], 0.0)
        fr = pltpu.matmul_pop(b0[slot])
        fi = pltpu.matmul_pop(b1[slot])
        img[j] = img[j] + w * (fr * fr + fi * fi)

    def block(i, carry):
        (j, b, n), (jp, bp, np_), seen = carry
        jn, bn, nn = place(jnp.minimum(i + 1, high - 1))
        seen = wait(bn, seen)
        data = half[...]
        for u in range(KB):
            if u + 2 < KB:
                stage_one(kbuf, both, a0, a1, j, b * KB + u + 2, u % 2)
            else:
                stage_one(kbuf, both, a0, a1, jn, bn * KB + (u + 2 - KB), u % 2)
            pltpu.matmul_acc_lhs(b0[u % 3], data)
            pltpu.matmul_acc_lhs(b1[u % 3], data)
            data = middle(a0, a1, (u + 1) % 2)
            if u < 2:
                finish(jp, bp * KB + KB - 2 + u, np_, (u + 1) % 3)
            else:
                finish(j, b * KB + u - 2, n, (u + 1) % 3)
        half[...] = data
        return (jn, bn, nn), (j, b, n), seen

    here = place(low)
    _, (j, b, n), seen = lax.fori_loop(low, high, block, (here, here, jnp.int32(0)))
    finish(j, b * KB + KB - 2, n, 1)
    finish(j, b * KB + KB - 1, n, 2)
    pltpu.matmul_pop(a0[1])
    pltpu.matmul_pop(a1[1])
    return seen, place


def stage_one(kbuf, both, a0, a1, j, k, slot, first=False):
    width = kbuf.shape[1]
    kb = kbuf[k].astype(jnp.float32)
    kr, ki = kb[:, :width], kb[:, width:]
    sp = both[j].astype(jnp.float32)
    sr, si = sp[:, :width], sp[:, width:]
    band = jnp.concatenate([kr * sr - ki * si, kr * si + ki * sr], 1).astype(jnp.bfloat16)
    load = 0 if first else None
    pltpu.matmul_acc_lhs(a0[slot], band, load_staged_rhs=load)
    pltpu.matmul_acc_lhs(a1[slot], band, load_staged_rhs=load)


def middle(a0, a1, slot):
    hr = pltpu.matmul_pop(a0[slot]).astype(jnp.bfloat16)
    hi = pltpu.matmul_pop(a1[slot]).astype(jnp.bfloat16)
    return jnp.concatenate([hr.T, hi.T], 1)


def push_table(tbuf, length):
    pltpu.matmul_push_rhs(tbuf[:, :length], staging_register=0, mxu_index=0)
    pltpu.matmul_push_rhs(tbuf[:, length:], staging_register=0, mxu_index=1)


def with_accs(body, width, length):
    pl.run_scoped(
        body,
        *[pltpu.ACC(0)((width, length), jnp.float32)] * 2,
        *[pltpu.ACC(1)((width, length), jnp.float32)] * 2,
        *[pltpu.ACC(0)((length, length), jnp.float32)] * 3,
        *[pltpu.ACC(1)((length, length), jnp.float32)] * 3,
    )


def first_kernel(pflags, pcounts, phelper, pspectra, flags, counts, helper, weights, kpart, tbuf, spectra, kernels,
                 img, kbuf, both, base, vertical, across, fl, cn, hm, pfl, pcn, phm, ws, half, ksem, sems):
    tiles, width, _ = spectra.shape
    length = img.shape[1]
    kern_total = kernels.shape[0]
    held = kpart.shape[0] // KB
    core = lax.rem(lax.axis_index("col"), 2)
    pairs = [(flags, fl), (counts, cn), (helper, hm), (pflags, pfl), (pcounts, pcn), (phelper, phm), (weights, ws)]
    copies = [pltpu.make_async_copy(src, dst, sems.at[i]) for i, (src, dst) in enumerate(pairs)]

    def chunk(b):
        part = pl.ds(b * KB, KB)
        return pltpu.make_async_copy(kernels.at[part], kbuf.at[part], ksem.at[b])

    for copy in copies:
        copy.start()
    for b in range(held, kern_total // KB):
        chunk(b).start()

    def body(*accs):
        for acc in accs:
            pltpu.matmul_pop(acc)
        push_table(tbuf, length)
        both[:tiles] = spectra[...]
        both[tiles:] = pspectra[...]
        kbuf[: kpart.shape[0]] = kpart[...]
        a0, a1 = accs[0:2], accs[2:4]
        j0 = lax.rem(core, tiles)
        stage_one(kbuf, both, a0, a1, j0, 0, 0, first=True)
        stage_one(kbuf, both, a0, a1, j0, 1, 1)
        half[...] = middle(a0, a1, 0)
        img[...] = jnp.zeros_like(img)
        for copy in copies:
            copy.wait()
        lists = plan(core, (fl, pfl), (cn, pcn), kern_total)
        total = lists[3][-1]
        split = split_of(total)

        def handed(f, h, direction):
            value = jnp.float32(0)
            for t in range(tiles):
                value = value + jnp.where((f[t] == 1) & (h[t] == direction), jnp.float32(kern_total), 0.0)
            return value

        odd_row = lax.rem(lax.axis_index("blk"), 2)
        direction = jnp.where(core == 0, 1 - odd_row, odd_row)
        mine, twins = handed(fl, hm, direction), handed(pfl, phm, direction)
        line = lax.broadcasted_iota(jnp.int32, vertical.shape, 0)
        vertical[...] = jnp.where(line == core, mine, jnp.where(line == 1 - core, twins, 0.0))
        across[...] = jnp.full(across.shape, handed(fl, hm, 3 - core))
        value = handed(pfl, phm, 3 - core)
        for t in range(tiles):
            value = value + jnp.where(fl[t] == 1, 0, cn[t]).astype(jnp.float32)
        base[...] = jnp.full(base.shape, value)

        def wait(b, seen):
            bit = lax.shift_left(jnp.int32(1), b)
            due = (b >= held) & ((seen & bit) == 0)

            @pl.when(due)
            def _():
                chunk(b).wait()

            return jnp.where(due, seen | bit, seen)

        seen, _ = run_part(jnp.int32(0), split, lists, kbuf, both, ws, img, half, accs, wait)

        def rest(b, seen):
            return wait(b, seen)

        lax.fori_loop(held, kern_total // KB, rest, seen)

    with_accs(body, width, length)


def second_kernel(pflags, pcounts, flags, counts, weights, kbuf, tbuf, both, img_in,
                  own_out, peer_out, fl, cn, pfl, pcn, ws, half, img, sems):
    tiles = own_out.shape[0]
    kern_total, width, _ = kbuf.shape
    length = img.shape[1]
    core = lax.rem(lax.axis_index("col"), 2)
    pairs = [(flags, fl), (counts, cn), (pflags, pfl), (pcounts, pcn), (weights, ws)]
    copies = [pltpu.make_async_copy(src, dst, sems.at[i]) for i, (src, dst) in enumerate(pairs)]
    for copy in copies:
        copy.start()

    def body(*accs):
        push_table(tbuf, length)
        for copy in copies:
            copy.wait()
        lists = plan(core, (fl, pfl), (cn, pcn), kern_total)
        total = lists[3][-1]
        low = split_of(total)
        a0, a1 = accs[0:2], accs[2:4]
        places, numbers, firsts, starts, _ = lists
        j, start, first = places[0], starts[0], firsts[0]
        for q in range(1, len(numbers)):
            take = low >= starts[q]
            j = jnp.where(take, places[q], j)
            start = jnp.where(take, starts[q], start)
            first = jnp.where(take, firsts[q], first)
        k = (first + 2 * (low - start)) * KB
        k = jnp.minimum(k, kern_total - KB)
        stage_one(kbuf, both, a0, a1, j, k, 0, first=True)
        stage_one(kbuf, both, a0, a1, j, k + 1, 1)
        half[...] = middle(a0, a1, 0)
        img[...] = img_in[...]
        run_part(low, total, lists, kbuf, both, ws, img, half, accs, lambda b, seen: seen)
        lane = lax.broadcasted_iota(jnp.int32, (1, kern_total), 1)
        for group, (f, c, dest) in enumerate(((fl, cn, own_out), (pfl, pcn, peer_out))):
            for t in range(tiles):
                n = jnp.where(f[t] == 1, kern_total, c[t])
                weight = jnp.sum(jnp.where(lane < n, weights[...], 0.0), axis=1, keepdims=True)
                dest[t] = img[group * tiles + t].T * (1.0 / weight)

    with_accs(body, width, length)


def final_kernel(scale, own, other, base, across, vertical, twins, image, pending):
    image[...] = own[...] + other[...]
    core = lax.rem(lax.axis_index("col"), 2)
    line = lax.broadcasted_iota(jnp.int32, base.shape, 0)
    both = jnp.where(line == core, vertical[...] + twins[...] + across[...] + base[...], 0.0)
    pending[...] = jnp.sum(both, axis=0, keepdims=True)[:, :1] * scale


def on_device(spectra, kernels, weights, hotspot_flags, helper_map, kernel_counts):
    tiles, width, _ = spectra.shape
    kern_total = kernels.shape[0]
    rows, cols = lax.axis_size("blk"), lax.axis_size("col")
    table = make_table(width, Q)

    def pairs(size, first):
        return [p for i in range(first, size, 2) for p in ((i, (i + 1) % size), ((i + 1) % size, i))]

    twin = pairs(cols, 0)
    pspectra = lax.ppermute(spectra, "col", twin)
    pflags = lax.ppermute(hotspot_flags, "col", twin)
    pcounts = lax.ppermute(kernel_counts, "col", twin)
    phelper = lax.ppermute(helper_map, "col", twin)

    vmem = pl.BlockSpec(memory_space=pltpu.VMEM)
    hbm = pl.BlockSpec(memory_space=pltpu.HBM)

    def far(*arrays):
        return [pltpu.with_memory_space_constraint(x, pltpu.HBM) for x in arrays]

    f32, bf16 = jnp.float32, jnp.bfloat16
    image = jax.ShapeDtypeStruct((tiles, Q, Q), f32)
    wide = jax.ShapeDtypeStruct((8, 128), f32)
    ints = pltpu.SMEM((tiles,), jnp.int32)
    params = pltpu.CompilerParams(vmem_limit_bytes=16 * 2**20)
    ivec = jax.ShapeDtypeStruct((tiles,), jnp.int32)
    fetch = pl.pallas_call(
        fetch_kernel,
        out_shape=[
            ivec,
            ivec,
            ivec,
            jax.ShapeDtypeStruct((1, kern_total), f32),
            jax.ShapeDtypeStruct((3 * KB, width, 2 * width), bf16),
            jax.ShapeDtypeStruct(table.shape, bf16),
            jax.ShapeDtypeStruct(spectra.shape, bf16),
        ],
        in_specs=[hbm] * 7,
        out_specs=[vmem] * 7,
        scratch_shapes=[pltpu.SemaphoreType.DMA((7,))],
        compiler_params=params,
        cost_estimate=pl.CostEstimate(flops=10**9, transcendentals=0, bytes_accessed=10**6),
        name="fetch",
    )
    fv, cv, hv, wv, kpart, tbuf, sbuf = fetch(
        *far(hotspot_flags, kernel_counts, helper_map, weights.reshape(1, -1), spectra, kernels, table)
    )
    row_smem = pltpu.SMEM((1, kern_total), f32)
    half = pltpu.VMEM((Q, 2 * width), bf16)
    images = jax.ShapeDtypeStruct((2 * tiles, Q, Q), f32)
    cost = pl.CostEstimate(flops=10**10, transcendentals=0, bytes_accessed=10**6)
    work = pl.pallas_call(
        first_kernel,
        out_shape=[
            images,
            jax.ShapeDtypeStruct(kernels.shape, bf16),
            jax.ShapeDtypeStruct((2 * tiles, width, 2 * width), bf16),
            wide,
            wide,
            wide,
        ],
        in_specs=[vmem] * 11 + [hbm],
        out_specs=[vmem] * 6,
        scratch_shapes=[
            *[ints] * 6,
            row_smem,
            half,
            pltpu.SemaphoreType.DMA((kern_total // KB,)),
            pltpu.SemaphoreType.DMA((7,)),
        ],
        compiler_params=params,
        cost_estimate=cost,
        name="work",
    )
    img, kbuf, both, base, vertical, across = work(
        pflags, pcounts, phelper, pspectra, fv, cv, hv, wv, kpart, tbuf, sbuf, *far(kernels)
    )
    rounds = []
    for parity in range(2):
        for i, j in pairs(rows, 1 - parity):
            rounds += [(i * cols + c, j * cols + c) for c in range(parity, cols, 2)]
    vertical = lax.ppermute(vertical, ("blk", "col"), rounds)
    across = lax.ppermute(across, "col", pairs(cols, 1))
    rest = pl.pallas_call(
        second_kernel,
        out_shape=[image, image],
        in_specs=[vmem] * 9,
        out_specs=[vmem] * 2,
        scratch_shapes=[
            *[ints] * 4,
            row_smem,
            half,
            pltpu.VMEM((2 * tiles, Q, Q), f32),
            pltpu.SemaphoreType.DMA((5,)),
        ],
        compiler_params=params,
        cost_estimate=cost,
        name="rest",
    )
    own, peer = rest(pflags, pcounts, fv, cv, wv, kbuf, tbuf, both, img)
    other = lax.ppermute(peer, "col", twin)
    twins = lax.ppermute(vertical, "col", twin)
    return tuple(
        pl.pallas_call(
            functools.partial(final_kernel, 1.0 / kern_total),
            out_shape=[image, jax.ShapeDtypeStruct((1, 1), f32)],
            in_specs=[vmem] * 6,
            out_specs=[vmem] * 2,
            compiler_params=params,
            name="final",
        )(own, other, base, across, vertical, twins)
    )


def solution(mesh):
    in_specs = (
        P(("blk", "col"), None, None),
        P(),
        P(),
        P(("blk", "col")),
        P(("blk", "col")),
        P(("blk", "col")),
    )
    out_specs = (P(("blk", "col"), None, None), P("blk", "col"))
    return jax.shard_map(on_device, mesh=mesh, in_specs=in_specs, out_specs=out_specs, check_vma=False)
```

```python
import functools
import math

import jax
import jax.numpy as jnp
import numpy as np
from jax import lax
from jax.experimental import pallas as pl
from jax.experimental.pallas import tpu as pltpu
from jax.sharding import PartitionSpec as P

Q = 256
KB = 6


def make_table(band_width, length):
    row_index = np.arange(length, dtype=np.int32)[:, None]
    col_index = np.arange(band_width, dtype=np.int32)[None, :] - band_width // 2
    angle = np.mod(row_index * col_index, length).astype(np.float64) * (2.0 * math.pi / length)
    scale = 1.0 / math.sqrt(band_width)
    real = (np.cos(angle) * scale).astype(np.float32).T
    imag = (np.sin(angle) * scale).astype(np.float32).T
    table = np.block([[real, imag], [-imag, real]])
    return jnp.asarray(table).astype(jnp.bfloat16)


def plan(core, flags, counts, kern_total):
    tiles, numbers, firsts, starts = [], [], [], [jnp.int32(0)]
    most = jnp.int32(0)
    for group, (f, c) in enumerate(zip(flags, counts)):
        per = f.shape[0]
        for q in range(per):
            t = lax.rem(core + q, per)
            n = jnp.where(f[t] == 1, kern_total, c[t])
            first = q % 2
            blocks = (n + KB - 1) // KB
            most = jnp.maximum(most, blocks)
            tiles.append(group * per + t)
            numbers.append(n)
            firsts.append(first)
            starts.append(starts[-1] + (blocks - first + 1) // 2)
    return tiles, numbers, firsts, starts, most


def fetch_kernel(flags, counts, helper, weights, spectra, kernels, table, fv, cv, hv, wv, kpart, tbuf, sbuf, sems):
    pairs = [(flags, fv), (counts, cv), (helper, hv), (weights, wv)]
    pairs += [(spectra, sbuf), (kernels.at[pl.ds(0, kpart.shape[0])], kpart), (table, tbuf)]
    copies = [pltpu.make_async_copy(src, dst, sems.at[i]) for i, (src, dst) in enumerate(pairs)]
    for copy in copies:
        copy.start()
    for copy in copies:
        copy.wait()


def split_of(total):
    return total - jnp.maximum((total - 2) // 2, 1)


def run_part(low, high, lists, kbuf, both, ws, img, half, accs, wait):
    a0, a1, b0, b1 = accs[0:2], accs[2:4], accs[4:7], accs[7:10]
    places, numbers, firsts, starts, _ = lists

    def place(i):
        j, start, first, n = places[0], starts[0], firsts[0], numbers[0]
        for q in range(1, len(numbers)):
            take = i >= starts[q]
            j = jnp.where(take, places[q], j)
            start = jnp.where(take, starts[q], start)
            first = jnp.where(take, firsts[q], first)
            n = jnp.where(take, numbers[q], n)
        return j, first + 2 * (i - start), n

    def finish(j, k, n, slot):
        w = jnp.where(k < n, ws[0, k], 0.0)
        fr = pltpu.matmul_pop(b0[slot])
        fi = pltpu.matmul_pop(b1[slot])
        img[j] = img[j] + w * (fr * fr + fi * fi)

    def block(i, carry):
        (j, b, n), (jp, bp, np_), seen = carry
        jn, bn, nn = place(jnp.minimum(i + 1, high - 1))
        seen = wait(bn, seen)
        data = half[...]
        for u in range(KB):
            if u + 2 < KB:
                stage_one(kbuf, both, a0, a1, j, b * KB + u + 2, u % 2)
            else:
                stage_one(kbuf, both, a0, a1, jn, bn * KB + (u + 2 - KB), u % 2)
            pltpu.matmul_acc_lhs(b0[u % 3], data)
            pltpu.matmul_acc_lhs(b1[u % 3], data)
            data = middle(a0, a1, (u + 1) % 2)
            if u < 2:
                finish(jp, bp * KB + KB - 2 + u, np_, (u + 1) % 3)
            else:
                finish(j, b * KB + u - 2, n, (u + 1) % 3)
        half[...] = data
        return (jn, bn, nn), (j, b, n), seen

    here = place(low)
    _, (j, b, n), seen = lax.fori_loop(low, high, block, (here, here, jnp.int32(0)))
    finish(j, b * KB + KB - 2, n, 1)
    finish(j, b * KB + KB - 1, n, 2)
    pltpu.matmul_pop(a0[1])
    pltpu.matmul_pop(a1[1])
    return seen, place


def stage_one(kbuf, both, a0, a1, j, k, slot, first=False):
    width = kbuf.shape[1]
    kb = kbuf[k].astype(jnp.float32)
    kr, ki = kb[:, :width], kb[:, width:]
    sp = both[j].astype(jnp.float32)
    sr, si = sp[:, :width], sp[:, width:]
    band = jnp.concatenate([kr * sr - ki * si, kr * si + ki * sr], 1).astype(jnp.bfloat16)
    load = 0 if first else None
    pltpu.matmul_acc_lhs(a0[slot], band, load_staged_rhs=load)
    pltpu.matmul_acc_lhs(a1[slot], band, load_staged_rhs=load)


def middle(a0, a1, slot):
    hr = pltpu.matmul_pop(a0[slot]).astype(jnp.bfloat16)
    hi = pltpu.matmul_pop(a1[slot]).astype(jnp.bfloat16)
    return jnp.concatenate([hr.T, hi.T], 1)


def push_table(tbuf, length):
    pltpu.matmul_push_rhs(tbuf[:, :length], staging_register=0, mxu_index=0)
    pltpu.matmul_push_rhs(tbuf[:, length:], staging_register=0, mxu_index=1)


def with_accs(body, width, length):
    pl.run_scoped(
        body,
        *[pltpu.ACC(0)((width, length), jnp.float32)] * 2,
        *[pltpu.ACC(1)((width, length), jnp.float32)] * 2,
        *[pltpu.ACC(0)((length, length), jnp.float32)] * 3,
        *[pltpu.ACC(1)((length, length), jnp.float32)] * 3,
    )


def first_kernel(pflags, pcounts, phelper, pspectra, flags, counts, helper, weights, kpart, tbuf, spectra, kernels,
                 img, kbuf, both, base, vertical, across, fl, cn, hm, pfl, pcn, phm, ws, half, ksem, sems):
    tiles, width, _ = spectra.shape
    length = img.shape[1]
    kern_total = kernels.shape[0]
    held = kpart.shape[0] // KB
    core = lax.rem(lax.axis_index("col"), 2)
    pairs = [(flags, fl), (counts, cn), (helper, hm), (pflags, pfl), (pcounts, pcn), (phelper, phm), (weights, ws)]
    copies = [pltpu.make_async_copy(src, dst, sems.at[i]) for i, (src, dst) in enumerate(pairs)]

    def chunk(b):
        part = pl.ds(b * KB, KB)
        return pltpu.make_async_copy(kernels.at[part], kbuf.at[part], ksem.at[b])

    for copy in copies:
        copy.start()
    for b in range(held, kern_total // KB):
        chunk(b).start()

    def body(*accs):
        for acc in accs:
            pltpu.matmul_pop(acc)
        push_table(tbuf, length)
        both[:tiles] = spectra[...]
        both[tiles:] = pspectra[...]
        kbuf[: kpart.shape[0]] = kpart[...]
        a0, a1 = accs[0:2], accs[2:4]
        j0 = lax.rem(core, tiles)
        stage_one(kbuf, both, a0, a1, j0, 0, 0, first=True)
        stage_one(kbuf, both, a0, a1, j0, 1, 1)
        half[...] = middle(a0, a1, 0)
        img[...] = jnp.zeros_like(img)
        for copy in copies:
            copy.wait()
        lists = plan(core, (fl, pfl), (cn, pcn), kern_total)
        total = lists[3][-1]
        split = split_of(total)

        def handed(f, h, direction):
            value = jnp.float32(0)
            for t in range(tiles):
                value = value + jnp.where((f[t] == 1) & (h[t] == direction), jnp.float32(kern_total), 0.0)
            return value

        odd_row = lax.rem(lax.axis_index("blk"), 2)
        direction = jnp.where(core == 0, 1 - odd_row, odd_row)
        mine, twins = handed(fl, hm, direction), handed(pfl, phm, direction)
        line = lax.broadcasted_iota(jnp.int32, vertical.shape, 0)
        vertical[...] = jnp.where(line == core, mine, jnp.where(line == 1 - core, twins, 0.0))
        across[...] = jnp.full(across.shape, handed(fl, hm, 3 - core))
        value = handed(pfl, phm, 3 - core)
        for t in range(tiles):
            value = value + jnp.where(fl[t] == 1, 0, cn[t]).astype(jnp.float32)
        base[...] = jnp.full(base.shape, value)

        def wait(b, seen):
            bit = lax.shift_left(jnp.int32(1), b)
            due = (b >= held) & ((seen & bit) == 0)

            @pl.when(due)
            def _():
                chunk(b).wait()

            return jnp.where(due, seen | bit, seen)

        seen, _ = run_part(jnp.int32(0), split, lists, kbuf, both, ws, img, half, accs, wait)

        def rest(b, seen):
            return wait(b, seen)

        lax.fori_loop(held, kern_total // KB, rest, seen)

    with_accs(body, width, length)


def second_kernel(pflags, pcounts, flags, counts, weights, kbuf, tbuf, both, img_in,
                  own_out, peer_out, fl, cn, pfl, pcn, ws, half, img, sems):
    tiles = own_out.shape[0]
    kern_total, width, _ = kbuf.shape
    length = img.shape[1]
    core = lax.rem(lax.axis_index("col"), 2)
    pairs = [(flags, fl), (counts, cn), (pflags, pfl), (pcounts, pcn), (weights, ws)]
    copies = [pltpu.make_async_copy(src, dst, sems.at[i]) for i, (src, dst) in enumerate(pairs)]
    for copy in copies:
        copy.start()

    def body(*accs):
        push_table(tbuf, length)
        for copy in copies:
            copy.wait()
        lists = plan(core, (fl, pfl), (cn, pcn), kern_total)
        total = lists[3][-1]
        low = split_of(total)
        a0, a1 = accs[0:2], accs[2:4]
        places, numbers, firsts, starts, _ = lists
        j, start, first = places[0], starts[0], firsts[0]
        for q in range(1, len(numbers)):
            take = low >= starts[q]
            j = jnp.where(take, places[q], j)
            start = jnp.where(take, starts[q], start)
            first = jnp.where(take, firsts[q], first)
        k = (first + 2 * (low - start)) * KB
        k = jnp.minimum(k, kern_total - KB)
        stage_one(kbuf, both, a0, a1, j, k, 0, first=True)
        stage_one(kbuf, both, a0, a1, j, k + 1, 1)
        half[...] = middle(a0, a1, 0)
        img[...] = img_in[...]
        run_part(low, total, lists, kbuf, both, ws, img, half, accs, lambda b, seen: seen)
        lane = lax.broadcasted_iota(jnp.int32, (1, kern_total), 1)
        for group, (f, c, dest) in enumerate(((fl, cn, own_out), (pfl, pcn, peer_out))):
            for t in range(tiles):
                n = jnp.where(f[t] == 1, kern_total, c[t])
                weight = jnp.sum(jnp.where(lane < n, weights[...], 0.0), axis=1, keepdims=True)
                dest[t] = (img[group * tiles + t].T * (1.0 / weight)).astype(dest.dtype)

    with_accs(body, width, length)


def final_kernel(scale, own, other, base, across, vertical, twins, image, pending):
    image[...] = own[...] + other[...].astype(own.dtype)
    core = lax.rem(lax.axis_index("col"), 2)
    line = lax.broadcasted_iota(jnp.int32, base.shape, 0)
    both = jnp.where(line == core, vertical[...] + twins[...] + across[...] + base[...], 0.0)
    pending[...] = jnp.sum(both, axis=0, keepdims=True)[:, :1] * scale


def on_device(spectra, kernels, weights, hotspot_flags, helper_map, kernel_counts):
    tiles, width, _ = spectra.shape
    kern_total = kernels.shape[0]
    rows, cols = lax.axis_size("blk"), lax.axis_size("col")
    table = make_table(width, Q)

    def pairs(size, first):
        return [p for i in range(first, size, 2) for p in ((i, (i + 1) % size), ((i + 1) % size, i))]

    twin = pairs(cols, 0)
    pspectra = lax.ppermute(spectra, "col", twin)
    pflags = lax.ppermute(hotspot_flags, "col", twin)
    pcounts = lax.ppermute(kernel_counts, "col", twin)
    phelper = lax.ppermute(helper_map, "col", twin)

    vmem = pl.BlockSpec(memory_space=pltpu.VMEM)
    hbm = pl.BlockSpec(memory_space=pltpu.HBM)

    def far(*arrays):
        return [pltpu.with_memory_space_constraint(x, pltpu.HBM) for x in arrays]

    f32, bf16 = jnp.float32, jnp.bfloat16
    image = jax.ShapeDtypeStruct((tiles, Q, Q), f32)
    wide = jax.ShapeDtypeStruct((8, 128), f32)
    ints = pltpu.SMEM((tiles,), jnp.int32)
    params = pltpu.CompilerParams(vmem_limit_bytes=16 * 2**20)
    ivec = jax.ShapeDtypeStruct((tiles,), jnp.int32)
    fetch = pl.pallas_call(
        fetch_kernel,
        out_shape=[
            ivec,
            ivec,
            ivec,
            jax.ShapeDtypeStruct((1, kern_total), f32),
            jax.ShapeDtypeStruct((2 * KB, width, 2 * width), bf16),
            jax.ShapeDtypeStruct(table.shape, bf16),
            jax.ShapeDtypeStruct(spectra.shape, bf16),
        ],
        in_specs=[hbm] * 7,
        out_specs=[vmem] * 7,
        scratch_shapes=[pltpu.SemaphoreType.DMA((7,))],
        compiler_params=params,
        cost_estimate=pl.CostEstimate(flops=10**9, transcendentals=0, bytes_accessed=10**6),
        name="fetch",
    )
    fv, cv, hv, wv, kpart, tbuf, sbuf = fetch(
        *far(hotspot_flags, kernel_counts, helper_map, weights.reshape(1, -1), spectra, kernels, table)
    )
    row_smem = pltpu.SMEM((1, kern_total), f32)
    half = pltpu.VMEM((Q, 2 * width), bf16)
    images = jax.ShapeDtypeStruct((2 * tiles, Q, Q), f32)
    cost = pl.CostEstimate(flops=10**10, transcendentals=0, bytes_accessed=10**6)
    work = pl.pallas_call(
        first_kernel,
        out_shape=[
            images,
            jax.ShapeDtypeStruct(kernels.shape, bf16),
            jax.ShapeDtypeStruct((2 * tiles, width, 2 * width), bf16),
            wide,
            wide,
            wide,
        ],
        in_specs=[vmem] * 11 + [hbm],
        out_specs=[vmem] * 6,
        scratch_shapes=[
            *[ints] * 6,
            row_smem,
            half,
            pltpu.SemaphoreType.DMA((kern_total // KB,)),
            pltpu.SemaphoreType.DMA((7,)),
        ],
        compiler_params=params,
        cost_estimate=cost,
        name="work",
    )
    img, kbuf, both, base, vertical, across = work(
        pflags, pcounts, phelper, pspectra, fv, cv, hv, wv, kpart, tbuf, sbuf, *far(kernels)
    )
    rounds = []
    for parity in range(2):
        for i, j in pairs(rows, 1 - parity):
            rounds += [(i * cols + c, j * cols + c) for c in range(parity, cols, 2)]
    vertical = lax.ppermute(vertical, ("blk", "col"), rounds)
    across = lax.ppermute(across, "col", pairs(cols, 1))
    rest = pl.pallas_call(
        second_kernel,
        out_shape=[image, jax.ShapeDtypeStruct(image.shape, bf16)],
        in_specs=[vmem] * 9,
        out_specs=[vmem] * 2,
        scratch_shapes=[
            *[ints] * 4,
            row_smem,
            half,
            pltpu.VMEM((2 * tiles, Q, Q), f32),
            pltpu.SemaphoreType.DMA((5,)),
        ],
        compiler_params=params,
        cost_estimate=cost,
        name="rest",
    )
    own, peer = rest(pflags, pcounts, fv, cv, wv, kbuf, tbuf, both, img)
    other = lax.ppermute(peer, "col", twin)
    twins = lax.ppermute(vertical, "col", twin)
    return tuple(
        pl.pallas_call(
            functools.partial(final_kernel, 1.0 / kern_total),
            out_shape=[image, jax.ShapeDtypeStruct((1, 1), f32)],
            in_specs=[vmem] * 6,
            out_specs=[vmem] * 2,
            compiler_params=params,
            name="final",
        )(own, other, base, across, vertical, twins)
    )


def solution(mesh):
    in_specs = (
        P(("blk", "col"), None, None),
        P(),
        P(),
        P(("blk", "col")),
        P(("blk", "col")),
        P(("blk", "col")),
    )
    out_specs = (P(("blk", "col"), None, None), P("blk", "col"))
    return jax.shard_map(on_device, mesh=mesh, in_specs=in_specs, out_specs=out_specs, check_vma=False)
```
